32 devices in a mesh: spin: 2 (over x), row: 4 (over z), col: 4 (over y, core).
Axes of the slice: x: 2, y: 2, z: 4, core: 2. Of those that a mesh axis runs over, the one named last changes fastest.
Arguments:
- hamiltonian: float32 [4096, 2048], P(('spin', 'row'), 'col'), parts along dimension 0
- bounds: float32 [4], P('spin'), parts along dimension 0
- occ_count: int32 [2], P('spin'), parts along dimension 0
- branches: int32 [12], P('spin'), parts along dimension 0
Outputs:
- output 1: float32 [4096, 2048], P(('spin', 'row'), 'col'), parts along dimension 0
- output 2: float32 [12], P('spin'), parts along dimension 0
- output 3: float32 [2], P('spin'), parts along dimension 0
There are 2 independent parts. The reference program is written for one: setup_inputs(seed, part) draws one part's arguments, and reference() takes and returns one part's arrays. A program takes and returns all parts, laid end to end along the dimension named above; each array names one.
All inputs are finite; a program needn't handle non-finite values.
Results may differ from the reference program's by a relative error of at most 0.001.
Values sent between devices are 32-bit elements.
A program may use at most 1 GiB of HBM per device.

```python
import jax
import jax.numpy as jnp
from jax import lax

N = 2048
STEPS = 6


def setup_inputs(seed: int = 0, part: int = 0) -> dict:
    base_key = jax.random.fold_in(jax.random.key(seed), part)
    key_ham, key_slack, key_occ, key_bits, key_perm = jax.random.split(base_key, 5)
    gauss_mat = jax.random.normal(key_ham, (N, N), jnp.float32)
    center = -2.0
    hamiltonian = (gauss_mat + gauss_mat.T) * (0.5 / N) ** 0.5 + center * jnp.eye(N, dtype=jnp.float32)
    slack_vals = jax.random.uniform(key_slack, (2,), jnp.float32, 0.1, 0.6)
    bounds = jnp.stack([center - 2.0 * (1.0 + slack_vals[0]), center + 2.0 * (1.0 + slack_vals[1])])
    occ_count = jax.random.randint(key_occ, (1,), (3 * N) // 20, (3 * N) // 8 + 1, jnp.int32)
    extra_bits = jax.random.randint(key_bits, (STEPS - 4,), 0, 2, jnp.int32)
    flag_pool = jnp.concatenate([jnp.zeros((2,), jnp.int32), jnp.ones((2,), jnp.int32), extra_bits])
    branches = jax.random.permutation(key_perm, flag_pool)
    return {"hamiltonian": hamiltonian, "bounds": bounds, "occ_count": occ_count, "branches": branches}


def reference(hamiltonian, bounds, occ_count, branches):
    identity = jnp.eye(N, dtype=jnp.float32)
    chem_pot = jnp.trace(hamiltonian) / N
    occupied = occ_count[0].astype(jnp.float32)
    scale_fac = jnp.minimum(occupied / (bounds[1] - chem_pot), (N - occupied) / (chem_pot - bounds[0]))
    density = (scale_fac / N) * (chem_pot * identity - hamiltonian) + (occupied / N) * identity

    def sp2_step(current, branch_flag):
        occupation = jnp.sum(current * current)
        squared = jnp.dot(current, current, preferred_element_type=jnp.float32)
        updated = jnp.where(branch_flag == 1, squared, 2.0 * current - squared)
        return updated, occupation

    density, occupations = lax.scan(sp2_step, density, branches)
    energy = 2.0 * jnp.sum(density * hamiltonian)
    return density, occupations, energy.reshape(1)
```

```python
import functools

import jax
import jax.numpy as jnp
from jax import lax
from jax.experimental import pallas as pl
from jax.experimental.pallas import tpu as pltpu
from jax.sharding import PartitionSpec as P

ORDERS = ((0, 1, 2), (1, 2, 0), (2, 0, 1))
F32 = jnp.float32


def neighbour(dim, row, col):
    if dim == 0:
        return row + 1 - 2 * (row % 2), col
    if dim == 1:
        return 3 - row, col
    return row, (col + 2) % 4


def thirds(rows):
    first = ((rows // 3 + 7) // 8) * 8
    sizes = (first, first, rows - 2 * first)
    return sizes, (0, first, 2 * first)


def kernel(steps, h_ref, bounds_ref, occ_ref, flag_ref, dens_ref, occs_ref, energy_ref, x_ref, stage, red, g_send, g_recv, f_send,
           f_recv, i_send, i_recv, d_send, d_recv, w_send, w_recv, r_send, r_recv, credit):
    block = h_ref.shape[0]
    half = block // 2
    order = 4 * block
    sizes, starts = thirds(half)
    spin, row, col = lax.axis_index("spin"), lax.axis_index("row"), lax.axis_index("col")
    core = col % 2
    partner = (row, col + 1 - 2 * core)
    odd = (row + col // 2) % 2

    def at(start, size):
        return pl.ds(pl.multiple_of(start, 8), size)

    def lanes(start, size):
        return pl.ds(pl.multiple_of(start, min(128, size)), size)

    def remote(src, dst, send, recv, where):
        return pltpu.make_async_remote_copy(
            src_ref=src, dst_ref=dst, send_sem=send, recv_sem=recv, device_id=(spin,) + tuple(where), device_id_type=pl.DeviceIdType.MESH
        )

    others = [(dr, dc) for dr in range(4) for dc in range(4) if dr or dc]
    barrier = pltpu.get_barrier_semaphore()
    for dr, dc in others:
        pl.semaphore_signal(
            barrier, inc=1, device_id=(spin, (row + dr) % 4, (col + dc) % 4), device_id_type=pl.DeviceIdType.MESH
        )
    pl.semaphore_wait(barrier, len(others))

    def quadrant(src, which):
        if which == 0:
            return 0, half
        if which == 2:
            return half, half
        low = jnp.where(src[0] > src[1], half, 0)
        return low, low

    def guarded(src, which, run):
        if which == 2:
            pl.when(src[0] == src[1])(run)
        else:
            run()

    def region(src, which, part):
        qr, qc = quadrant(src, which)
        return x_ref.at[1, at(src[0] * block + qr + starts[part], sizes[part]), lanes(src[1] * block + qc, half)]

    def own_region(which, part):
        qr, qc = quadrant((row, col), which)
        return h_ref.at[at(qr + starts[part], sizes[part]), lanes(qc, half)]

    x_ref[1, at(row * block, block), lanes(col * block, block)] = h_ref[...]
    stage[...] = jnp.zeros_like(stage)

    def gather_index(part, slot, which):
        return (part * 7 + slot) * 3 + which

    def forward_index(part, slot, which):
        return (part * 8 + slot) * 3 + which

    held = [[(row, col)] for _ in ORDERS]
    for part in range(3):
        for which in range(3):
            n = forward_index(part, 7, which)
            guarded((row, col), which, lambda part=part, which=which, n=n: remote(
                own_region(which, part), region((row, col), which, part), f_send.at[n], f_recv.at[n], partner).start())
    for phase in range(3):
        base = (1 << phase) - 1
        for part, dims in enumerate(ORDERS):
            target = neighbour(dims[phase], row, col)
            for k, src in enumerate(held[part]):
                for which in range(3):
                    n = gather_index(part, base + k, which)
                    source = own_region(which, part) if k == 0 else region(src, which, part)
                    guarded(src, which, lambda source=source, src=src, which=which, part=part, n=n, target=target: remote(
                        source, region(src, which, part), g_send.at[n], g_recv.at[n], target).start())
        for part, dims in enumerate(ORDERS):
            target = neighbour(dims[phase], row, col)
            fresh = [neighbour(dims[phase], *src) for src in held[part]]
            for k, src in enumerate(fresh):
                for which in range(3):
                    n = gather_index(part, base + k, which)
                    m = forward_index(part, base + k, which)

                    def arrive(src=src, which=which, part=part, n=n, m=m, target=target):
                        spot = region(src, which, part)
                        remote(spot, spot, g_send.at[n], g_recv.at[n], target).wait_recv()
                        remote(spot, spot, f_send.at[m], f_recv.at[m], partner).start()

                    guarded(src, which, arrive)
            held[part] = held[part] + fresh
    for part, dims in enumerate(ORDERS):
        for slot in range(8):
            mine = held[part][(slot + 1) % 8]
            theirs = (mine[0], mine[1] + 1 - 2 * core)
            for which in range(3):
                m = forward_index(part, slot, which)

                def settle(theirs=theirs, which=which, part=part, m=m):
                    spot = region(theirs, which, part)
                    remote(spot, spot, f_send.at[m], f_recv.at[m], partner).wait_recv()

                guarded(theirs, which, settle)

                def drain(mine=mine, which=which, part=part, m=m):
                    spot = region(mine, which, part)
                    remote(spot, spot, f_send.at[m], f_recv.at[m], partner).wait_send()

                guarded(mine, which, drain)
    for phase in range(3):
        base = (1 << phase) - 1
        for part, dims in enumerate(ORDERS):
            for k, src in enumerate(held[part][: 1 << phase]):
                for which in range(3):
                    n = gather_index(part, base + k, which)

                    def drain(src=src, which=which, part=part, n=n):
                        spot = region(src, which, part)
                        remote(spot, spot, g_send.at[n], g_recv.at[n], partner).wait_send()

                    guarded(src, which, drain)

    quad_eye = lax.broadcasted_iota(jnp.int32, (half, half), 0) == lax.broadcasted_iota(jnp.int32, (half, half), 1)
    trace = jnp.zeros((half, half), F32)
    for k in range(8):
        trace = trace + x_ref[1, k * half:(k + 1) * half, k * half:(k + 1) * half]
    trace = jnp.where(quad_eye, trace, 0.0)
    chem = jnp.sum(jnp.sum(trace, axis=0, keepdims=True), axis=1, keepdims=True) / order
    occupied = jnp.full((1, 1), occ_ref[0], jnp.int32).astype(F32)
    scale = jnp.minimum(occupied / (bounds_ref[1] - chem), (order - occupied) / (chem - bounds_ref[0])) / order
    shift = occupied / order

    def convert(n, carry):
        i, j = n // 4, n % 4
        low = jnp.where(i > j, half, 0)

        def one(qr, qc):
            eye = jnp.logical_and(quad_eye, i * block + qr == j * block + qc)
            value = x_ref[1, at(i * block + qr, half), lanes(j * block + qc, half)]
            value = scale * (jnp.where(eye, chem, 0.0) - value) + jnp.where(eye, shift, 0.0)
            x_ref[0, at(i * block + qr, half), lanes(j * block + qc, half)] = value
            x_ref[0, at(j * block + qc, half), lanes(i * block + qr, half)] = value.T

        one(0, half)
        one(low, low)

        @pl.when(i == j)
        def _():
            one(half, half)

        return carry

    lax.fori_loop(0, 16, convert, 0)

    def sigma(flip, i):
        return i + flip * (3 - 2 * i)

    def piece_at(flip, who, k):
        diag = k // 2
        i = sigma(flip, diag * who)
        j = sigma(flip, diag * who + (1 - diag) * (1 + who))
        return i * block + (k % 2) * half, j * block

    def product(cur, r0, c0, height, width, flag):
        got = jnp.dot(
            x_ref[cur, at(r0, height), :], x_ref[cur, :, lanes(c0, width)], precision=lax.Precision.HIGHEST, preferred_element_type=F32
        )
        old = x_ref[cur, at(r0, height), lanes(c0, width)]
        return jnp.where(flag == 1, got, 2.0 * old - got)

    def signal_credit():
        for dim in range(3):
            pl.semaphore_signal(credit.at[dim], inc=1, device_id=(spin,) + neighbour(dim, row, col), device_id_type=pl.DeviceIdType.MESH)
        pl.semaphore_signal(credit.at[3], inc=1, device_id=(spin,) + partner, device_id_type=pl.DeviceIdType.MESH)

    def squares(cur):
        own = x_ref[cur, at(row * block, block), lanes(col * block, block)]
        return lane_sums(own * own)

    def lane_sums(value):
        total = value[:, :128]
        for k in range(1, block // 128):
            total = total + value[:, k * 128:(k + 1) * 128]
        return jnp.sum(total, axis=0, keepdims=True)

    def step(t, carry):
        cur, nxt = t % 2, 1 - t % 2
        flag = flag_ref[t]
        stage[pl.ds(t, 1), :] = squares(cur)

        def rect(r0, c0, height, width):
            return x_ref.at[nxt, at(r0, height), lanes(c0, width)]

        def to_partner(spot, n):
            return remote(spot, spot, d_send.at[n], d_recv.at[n], partner)

        def third(flip, who, k, part, width):
            r0, c0 = piece_at(flip, who, k)
            c0 = c0 if width == block else c0 + half
            return rect(r0 + starts[part], c0, sizes[part], width)

        def width_of(k):
            return half if isinstance(k, int) and k == 3 else block

        def outward(k):
            return [remote(third(odd, core, k, d, width_of(k)), third(odd, core, k, d, width_of(k)), i_send.at[k * 3 + d], i_recv.at[k * 3 + d],
                           neighbour(d, row, col)) for d in range(3)]

        def inward(k):
            return [remote(third(1 - odd, core, k, d, width_of(k)), third(1 - odd, core, k, d, width_of(k)), i_send.at[k * 3 + d],
                           i_recv.at[k * 3 + d], neighbour(d, row, col)) for d in range(3)]

        def passed(who, k):
            return [remote(third(1 - odd, who, k, d, width_of(k)), third(1 - odd, who, k, d, width_of(k)), w_send.at[k * 3 + d],
                           w_recv.at[k * 3 + d], partner) for d in range(3)]

        def local_copies(who, k, whole):
            r0, c0 = piece_at(odd, who, k)
            spots = [rect(r0, c0, half, block), rect(c0 + half, r0, half, half)] + ([rect(c0, r0, half, half)] if whole else [])
            return [to_partner(spot, k * 3 + n) for n, spot in enumerate(spots)]

        def last_quadrant(who):
            r0, c0 = piece_at(odd, who, 3)
            return to_partner(rect(r0, c0 + half, half, half), 9)

        def shared(who):
            r0, c0 = sigma(odd, who) * block, sigma(odd, 3 - who) * block
            return [to_partner(rect(r0, c0, block, block), 10), to_partner(rect(c0, r0, block, block), 11)]

        def piece(k, carry):
            r0, c0 = piece_at(odd, core, k)
            new = product(cur, r0, c0, half, block, flag)

            @pl.when(k == 0)
            def _():
                for n in range(4):
                    pl.semaphore_wait(credit.at[n], 1)

            x_ref[nxt, at(r0, half), lanes(c0, block)] = new
            x_ref[nxt, at(c0, block), lanes(r0, half)] = new.T
            for copy in outward(k):
                copy.start()
            for copy in local_copies(core, k, False):
                copy.start()

            @pl.when(k < 2)
            def _():
                local_copies(core, k, True)[2].start()

            return carry

        def relay(k):
            for arrived, onward in zip(inward(k), passed(core, k)):
                arrived.wait_recv()
                onward.start()

        lax.fori_loop(0, 3, piece, 0)
        relay(0)
        r0, c0 = piece_at(odd, core, 3)
        x_ref[nxt, at(r0, half), lanes(c0 + half, half)] = product(cur, r0, c0 + half, half, half, flag)
        for copy in outward(3):
            copy.start()
        last_quadrant(core).start()
        relay(1)
        r0, c0 = sigma(odd, core) * block, sigma(odd, 3 - core) * block
        new = product(cur, r0, c0, block, block, flag)
        x_ref[nxt, at(r0, block), lanes(c0, block)] = new
        x_ref[nxt, at(c0, block), lanes(r0, block)] = new.T
        for copy in shared(core):
            copy.start()
        relay(2)
        relay(3)

        for k in range(3):
            for copy in local_copies(1 - core, k, k < 2):
                copy.wait_recv()
        last_quadrant(1 - core).wait_recv()
        for copy in shared(1 - core):
            copy.wait_recv()
        for k in range(4):
            for copy in passed(1 - core, k):
                copy.wait_recv()

        def mirror(n, carry):
            k, who = n // 2, n % 2
            r0, c0 = piece_at(1 - odd, who, k)
            x_ref[nxt, at(c0 + half, half), lanes(r0, half)] = x_ref[nxt, at(r0, half), lanes(c0 + half, half)].T

            @pl.when(k < 2)
            def _():
                x_ref[nxt, at(c0, half), lanes(r0, half)] = x_ref[nxt, at(r0, half), lanes(c0, half)].T

            return carry

        for k in range(4):
            for copy in outward(k) + passed(core, k):
                copy.wait_send()
        for k in range(3):
            for copy in local_copies(core, k, k < 2):
                copy.wait_send()
        last_quadrant(core).wait_send()
        for copy in shared(core):
            copy.wait_send()
        lax.fori_loop(0, 6, mirror, 0)

        @pl.when(t < steps - 2)
        def _():
            signal_credit()

        return carry

    signal_credit()
    lax.fori_loop(0, steps - 1, step, 0)

    last = (steps - 1) % 2
    stage[steps - 1:steps, :] = squares(last)
    final = product(last, row * block, col * block, block, block, flag_ref[steps - 1])
    dens_ref[...] = final
    stage[steps:steps + 1, :] = lane_sums(final * h_ref[...])

    red[row * 4 + col] = stage[...]
    for n, (dr, dc) in enumerate(others):
        remote(stage, red.at[row * 4 + col], r_send.at[n], r_recv.at[n], ((row + dr) % 4, (col + dc) % 4)).start()
    for n, (dr, dc) in enumerate(others):
        spot = red.at[((row - dr) % 4) * 4 + (col - dc) % 4]
        remote(stage, spot, r_send.at[n], r_recv.at[n], partner).wait_recv()
    total = red[0]
    for n in range(1, 16):
        total = total + red[n]
    for n in range(steps):
        occs_ref[n] = jnp.sum(total[n:n + 1, :])
    energy_ref[0] = 2.0 * jnp.sum(total[steps:steps + 1, :])
    for n, (dr, dc) in enumerate(others):
        remote(stage, red.at[row * 4 + col], r_send.at[n], r_recv.at[n], ((row + dr) % 4, (col + dc) % 4)).wait_send()


def solution(mesh):
    def local_run(ham_block, bounds, occ_count, branches):
        block, steps = ham_block.shape[0], branches.shape[0]
        order = 4 * block
        dma = pltpu.SemaphoreType.DMA
        vmem = pl.BlockSpec(memory_space=pltpu.VMEM)
        smem = pl.BlockSpec(memory_space=pltpu.SMEM)
        return pl.pallas_call(
            functools.partial(kernel, steps),
            out_shape=(
                jax.ShapeDtypeStruct((block, block), F32),
                jax.ShapeDtypeStruct((steps,), F32),
                jax.ShapeDtypeStruct((1,), F32),
            ),
            in_specs=[vmem, smem, smem, smem],
            out_specs=(vmem, smem, smem),
            scratch_shapes=[
                pltpu.VMEM((2, order, order), F32),
                pltpu.VMEM((8, 128), F32),
                pltpu.VMEM((16, 8, 128), F32),
                dma((63,)), dma((63,)), dma((72,)), dma((72,)),
                dma((12,)), dma((12,)), dma((12,)), dma((12,)), dma((12,)), dma((12,)),
                dma((15,)), dma((15,)),
                pltpu.SemaphoreType.REGULAR((4,)),
            ],
            compiler_params=pltpu.CompilerParams(collective_id=0, has_side_effects=True, vmem_limit_bytes=60 * 1024 * 1024),
        )(ham_block, bounds, occ_count, branches)

    return jax.shard_map(
        local_run,
        mesh=mesh,
        in_specs=(P(("spin", "row"), "col"), P("spin"), P("spin"), P("spin")),
        out_specs=(P(("spin", "row"), "col"), P("spin"), P("spin")),
        check_vma=False,
    )
```

```python
import functools

import jax
import jax.numpy as jnp
from jax import lax
from jax.experimental import pallas as pl
from jax.experimental.pallas import tpu as pltpu
from jax.sharding import PartitionSpec as P

F32 = jnp.float32


def neighbour(dim, row, col):
    if dim == 0:
        return row + 1 - 2 * (row % 2), col
    return row, (col + 2) % 4


def kernel(steps, h_ref, bounds_ref, occ_ref, flag_ref, dens_ref, occs_ref, energy_ref, x_ref, stage, red, z_send, z_recv, y_send,
           y_recv, f_send, f_recv, i_send, i_recv, d_send, d_recv, w_send, w_recv, r_send, r_recv, credit):
    block = h_ref.shape[0]
    half = block // 2
    order = 4 * block
    spin, row, col = lax.axis_index("spin"), lax.axis_index("row"), lax.axis_index("col")
    core = col % 2
    partner = (row, col + 1 - 2 * core)
    odd = (row + col // 2) % 2

    def at(start, size):
        return pl.ds(pl.multiple_of(start, 8), size)

    def lanes(start, size):
        return pl.ds(pl.multiple_of(start, min(128, size)), size)

    def remote(src, dst, send, recv, where):
        return pltpu.make_async_remote_copy(
            src_ref=src, dst_ref=dst, send_sem=send, recv_sem=recv, device_id=(spin,) + tuple(where), device_id_type=pl.DeviceIdType.MESH
        )

    others = [(dr, dc) for dr in range(4) for dc in range(4) if dr or dc]
    barrier = pltpu.get_barrier_semaphore()
    for dr, dc in others:
        pl.semaphore_signal(
            barrier, inc=1, device_id=(spin, (row + dr) % 4, (col + dc) % 4), device_id_type=pl.DeviceIdType.MESH
        )
    pl.semaphore_wait(barrier, len(others))

    def guarded(src, which, run):
        if which == 2:
            pl.when(src[0] == src[1])(run)
        else:
            run()

    def quadrant(src, which):
        low = jnp.where(src[0] > src[1], half, 0)
        return ((0, half), (low, low), (half, half))[which]

    def region(src, which):
        qr, qc = quadrant(src, which)
        return x_ref.at[1, at(src[0] * block + qr, half), lanes(src[1] * block + qc, half)]

    def own_region(which):
        qr, qc = quadrant((row, col), which)
        return h_ref.at[at(qr, half), lanes(qc, half)]

    def each(src, run):
        for which in range(3):
            guarded(src, which, functools.partial(run, which))

    x_ref[1, at(row * block, block), lanes(col * block, block)] = h_ref[...]
    stage[...] = jnp.zeros_like(stage)
    across = (row, (col + 2) % 4)
    rows = (row, row + 1 - 2 * (row % 2), (row + 2) % 4, 3 - row)
    mine = [(r, col) for r in rows]
    theirs = [(r, across[1]) for r in rows]

    def z_out(k, which):
        spot = region(mine[0], which)
        return remote(own_region(which), spot, z_send.at[3 * k + which], z_recv.at[3 * k + which], mine[k])

    def z_in(k, which):
        spot = region(mine[k], which)
        return remote(spot, spot, z_send.at[3 * k + which], z_recv.at[3 * k + which], mine[k])

    def y_out(k, which):
        spot = region(mine[k], which)
        return remote(own_region(which) if k == 0 else spot, spot, y_send.at[3 * k + which], y_recv.at[3 * k + which], across)

    def y_in(k, which):
        spot = region(theirs[k], which)
        return remote(spot, spot, y_send.at[3 * k + which], y_recv.at[3 * k + which], across)

    def f_out(k, which):
        src = (mine + theirs)[k]
        spot = region(src, which)
        return remote(own_region(which) if k == 0 else spot, spot, f_send.at[3 * k + which], f_recv.at[3 * k + which], partner)

    def f_in(k, which):
        src = (mine + theirs)[k]
        spot = region((src[0], src[1] + 1 - 2 * core), which)
        return remote(spot, spot, f_send.at[3 * k + which], f_recv.at[3 * k + which], partner)

    each(mine[0], lambda which: y_out(0, which).start())
    for k in (1, 2, 3):
        each(mine[0], lambda which, k=k: z_out(k, which).start())
    each(mine[0], lambda which: f_out(0, which).start())
    for k in range(4):
        if k:
            def arrived(which, k=k):
                z_in(k, which).wait_recv()
                y_out(k, which).start()
                f_out(k, which).start()

            each(mine[k], arrived)

        def crossed(which, k=k):
            y_in(k, which).wait_recv()
            f_out(4 + k, which).start()

        each(theirs[k], crossed)
    for k in range(8):
        each(((mine + theirs)[k][0], (mine + theirs)[k][1] + 1 - 2 * core), lambda which, k=k: f_in(k, which).wait_recv())
    for k in range(8):
        each((mine + theirs)[k], lambda which, k=k: f_out(k, which).wait_send())
    for k in range(4):
        each(mine[k], lambda which, k=k: y_out(k, which).wait_send())
    for k in (1, 2, 3):
        each(mine[0], lambda which, k=k: z_out(k, which).wait_send())

    quad_eye = lax.broadcasted_iota(jnp.int32, (half, half), 0) == lax.broadcasted_iota(jnp.int32, (half, half), 1)
    trace = jnp.zeros((half, half), F32)
    for k in range(8):
        trace = trace + x_ref[1, k * half:(k + 1) * half, k * half:(k + 1) * half]
    trace = jnp.where(quad_eye, trace, 0.0)
    chem = jnp.sum(jnp.sum(trace, axis=0, keepdims=True), axis=1, keepdims=True) / order
    occupied = jnp.full((1, 1), occ_ref[0], jnp.int32).astype(F32)
    scale = jnp.minimum(occupied / (bounds_ref[1] - chem), (order - occupied) / (chem - bounds_ref[0])) / order
    shift = occupied / order

    def convert(n, carry):
        i, j = n // 4, n % 4
        low = jnp.where(i > j, half, 0)

        def one(qr, qc):
            eye = jnp.logical_and(quad_eye, i * block + qr == j * block + qc)
            value = x_ref[1, at(i * block + qr, half), lanes(j * block + qc, half)]
            value = scale * (jnp.where(eye, chem, 0.0) - value) + jnp.where(eye, shift, 0.0)
            x_ref[0, at(i * block + qr, half), lanes(j * block + qc, half)] = value
            x_ref[0, at(j * block + qc, half), lanes(i * block + qr, half)] = value.T

        one(0, half)
        one(low, low)

        @pl.when(i == j)
        def _():
            one(half, half)

        return carry

    lax.fori_loop(0, 16, convert, 0)

    def sigma(flip, i):
        return i + flip * (3 - 2 * i)

    def between(flip, who):
        return sigma(flip, 0) * block + who * half, sigma(flip, 1) * block

    def product(cur, r0, c0, height, width, flag):
        got = jnp.dot(
            x_ref[cur, at(r0, height), :], x_ref[cur, :, lanes(c0, width)], precision=lax.Precision.HIGHEST, preferred_element_type=F32
        )
        old = x_ref[cur, at(r0, height), lanes(c0, width)]
        return jnp.where(flag == 1, got, 2.0 * old - got)

    near = (neighbour(0, row, col), neighbour(2, row, col))
    sources = near + (partner,)

    def signal_credit():
        for n, where in enumerate(sources):
            pl.semaphore_signal(credit.at[n], inc=1, device_id=(spin,) + where, device_id_type=pl.DeviceIdType.MESH)

    def take_credit():
        for n in range(3):
            pl.semaphore_wait(credit.at[n], 1)

    def lane_sums(value):
        total = value[:, :128]
        for k in range(1, block // 128):
            total = total + value[:, k * 128:(k + 1) * 128]
        return jnp.sum(total, axis=0, keepdims=True)

    def squares(cur):
        own = x_ref[cur, at(row * block, block), lanes(col * block, block)]
        return lane_sums(own * own)

    quarter = half // 2

    def rect(slot, r0, c0, height, width):
        return x_ref.at[slot, at(r0, height), lanes(c0, width)]

    def piece(flip, who, k):
        d0 = sigma(flip, who) * block
        if k == 0:
            return d0, d0, block
        if k == 1:
            return d0 + half, d0 + half, half
        return between(flip, who) + (block,)

    def part_copy(flip, who, k, part, slot, send, recv, where):
        r0, c0, width = piece(flip, who, k)
        spot = rect(slot, r0 + part * quarter, c0, quarter, width)
        n = slot * 6 + k * 2 + part
        return remote(spot, spot, send.at[n], recv.at[n], where)

    def outward(k, part, slot):
        return part_copy(odd, core, k, part, slot, i_send, i_recv, near[part])

    def inward(k, part, slot):
        return part_copy(1 - odd, core, k, part, slot, i_send, i_recv, near[part])

    def passed(who, k, part, slot):
        return part_copy(1 - odd, who, k, part, slot, w_send, w_recv, partner)

    def direct(who, k, slot):
        if k < 3:
            r0, c0, width = piece(odd, who, k)
            if k == 0:
                spots = [rect(slot, r0, c0, half, block), rect(slot, c0 + half, r0, half, half)]
            elif k == 1:
                spots = [rect(slot, r0, c0, half, half)]
            else:
                spots = [rect(slot, r0, c0, half, block), rect(slot, c0, r0, block, half)]
        else:
            r0, c0 = sigma(odd, who) * block, sigma(odd, k - 1) * block
            spots = [rect(slot, r0, c0, block, block), rect(slot, c0, r0, block, block)]
        return [remote(spot, spot, d_send.at[slot * 10 + 2 * k + n], d_recv.at[slot * 10 + 2 * k + n], partner) for n, spot in enumerate(spots)]

    def send_piece(k, slot):
        for part in range(2):
            outward(k, part, slot).start()
        for copy in direct(core, k, slot):
            copy.start()

    def relay(k, slot):
        for part in range(2):
            inward(k, part, slot).wait_recv()
            passed(core, k, part, slot).start()

    def partner_settled(slot):
        for k in (0, 1, 3, 4):
            for copy in direct(1 - core, k, slot):
                copy.wait_recv()

    def remote_settled(slot):
        for k in range(3):
            for part in range(2):
                passed(1 - core, k, part, slot).wait_recv()
        for who in range(2):
            r0, c0, _ = piece(1 - odd, who, 0)
            x_ref[slot, at(c0 + half, half), lanes(r0, half)] = x_ref[slot, at(r0, half), lanes(c0 + half, half)].T
            r0, c0, _ = piece(1 - odd, who, 2)
            x_ref[slot, at(c0, block), lanes(r0, half)] = x_ref[slot, at(r0, half), lanes(c0, block)].T

    def drained(slot):
        for k in range(5):
            for copy in direct(core, k, slot):
                copy.wait_send()
        for k in range(3):
            for part in range(2):
                outward(k, part, slot).wait_send()
                passed(core, k, part, slot).wait_send()

    def step(t, carry):
        cur, nxt = t % 2, 1 - t % 2
        flag = flag_ref[t]

        r0, c0, _ = piece(odd, core, 0)
        new = product(cur, r0, c0, half, block, flag)
        take_credit()
        x_ref[nxt, at(r0, half), lanes(c0, block)] = new
        x_ref[nxt, at(c0 + half, half), lanes(r0, half)] = new[:, half:].T
        send_piece(0, nxt)

        r0, c0, _ = piece(odd, core, 1)
        x_ref[nxt, at(r0, half), lanes(c0, half)] = product(cur, r0, c0, half, half, flag)
        send_piece(1, nxt)

        @pl.when(t > 0)
        def _():
            partner_settled(cur)

        r0, c0, _ = piece(odd, core, 2)
        new = product(cur, r0, c0, half, block, flag)
        x_ref[nxt, at(r0, half), lanes(c0, block)] = new
        x_ref[nxt, at(c0, block), lanes(r0, half)] = new.T
        send_piece(2, nxt)

        @pl.when(t > 0)
        def _():
            remote_settled(cur)

        stage[pl.ds(t, 1), :] = squares(cur)

        def wide(k, carry):
            r0, c0 = sigma(odd, core) * block, sigma(odd, 2 + k) * block
            new = product(cur, r0, c0, block, block, flag)
            x_ref[nxt, at(r0, block), lanes(c0, block)] = new
            x_ref[nxt, at(c0, block), lanes(r0, block)] = new.T

            @pl.when(k == 0)
            def _():
                for copy in direct(core, 3, nxt):
                    copy.start()
                relay(0, nxt)
                relay(1, nxt)

            return carry

        lax.fori_loop(0, 2, wide, 0)
        for copy in direct(core, 4, nxt):
            copy.start()
        relay(2, nxt)
        for copy in direct(1 - core, 2, nxt):
            copy.wait_recv()

        @pl.when(t > 0)
        def _():
            drained(cur)

        @pl.when(t < steps - 2)
        def _():
            signal_credit()

        return carry

    signal_credit()
    lax.fori_loop(0, steps - 1, step, 0)
    last = (steps - 1) % 2
    partner_settled(last)
    remote_settled(last)

    stage[steps - 1:steps, :] = squares(last)
    final = product(last, row * block, col * block, block, block, flag_ref[steps - 1])
    dens_ref[...] = final
    drained(last)
    stage[steps:steps + 1, :] = lane_sums(final * h_ref[...])

    red[row * 4 + col] = stage[...]
    for n, (dr, dc) in enumerate(others):
        remote(stage, red.at[row * 4 + col], r_send.at[n], r_recv.at[n], ((row + dr) % 4, (col + dc) % 4)).start()
    for n, (dr, dc) in enumerate(others):
        spot = red.at[((row - dr) % 4) * 4 + (col - dc) % 4]
        remote(stage, spot, r_send.at[n], r_recv.at[n], partner).wait_recv()
    total = red[0]
    for n in range(1, 16):
        total = total + red[n]
    for n in range(steps):
        occs_ref[n] = jnp.sum(total[n:n + 1, :])
    energy_ref[0] = 2.0 * jnp.sum(total[steps:steps + 1, :])
    for n, (dr, dc) in enumerate(others):
        remote(stage, red.at[row * 4 + col], r_send.at[n], r_recv.at[n], ((row + dr) % 4, (col + dc) % 4)).wait_send()


def solution(mesh):
    def local_run(ham_block, bounds, occ_count, branches):
        block, steps = ham_block.shape[0], branches.shape[0]
        order = 4 * block
        dma = pltpu.SemaphoreType.DMA
        vmem = pl.BlockSpec(memory_space=pltpu.VMEM)
        smem = pl.BlockSpec(memory_space=pltpu.SMEM)
        return pl.pallas_call(
            functools.partial(kernel, steps),
            out_shape=(
                jax.ShapeDtypeStruct((block, block), F32),
                jax.ShapeDtypeStruct((steps,), F32),
                jax.ShapeDtypeStruct((1,), F32),
            ),
            in_specs=[vmem, smem, smem, smem],
            out_specs=(vmem, smem, smem),
            scratch_shapes=[
                pltpu.VMEM((2, order, order), F32),
                pltpu.VMEM((8, 128), F32),
                pltpu.VMEM((16, 8, 128), F32),
                dma((12,)), dma((12,)), dma((12,)), dma((12,)), dma((24,)), dma((24,)),
                dma((12,)), dma((12,)), dma((20,)), dma((20,)), dma((12,)), dma((12,)),
                dma((15,)), dma((15,)),
                pltpu.SemaphoreType.REGULAR((3,)),
            ],
            compiler_params=pltpu.CompilerParams(collective_id=0, has_side_effects=True, vmem_limit_bytes=60 * 1024 * 1024),
        )(ham_block, bounds, occ_count, branches)

    return jax.shard_map(
        local_run,
        mesh=mesh,
        in_specs=(P(("spin", "row"), "col"), P("spin"), P("spin"), P("spin")),
        out_specs=(P(("spin", "row"), "col"), P("spin"), P("spin")),
        check_vma=False,
    )
```

```python
import functools

import jax
import jax.numpy as jnp
from jax import lax
from jax.experimental import pallas as pl
from jax.experimental.pallas import tpu as pltpu
from jax.sharding import PartitionSpec as P

F32 = jnp.float32


def neighbour(dim, row, col):
    if dim == 0:
        return row + 1 - 2 * (row % 2), col
    return row, (col + 2) % 4


def kernel(steps, h_ref, bounds_ref, occ_ref, flag_ref, dens_ref, occs_ref, energy_ref, x_ref, stage, red, z_send, z_recv, e_send,
           e_recv, y_send, y_recv, f_send, f_recv, i_send, i_recv, d_send, d_recv, w_send, w_recv, r_send, r_recv, credit):
    block = h_ref.shape[0]
    half = block // 2
    order = 4 * block
    spin, row, col = lax.axis_index("spin"), lax.axis_index("row"), lax.axis_index("col")
    core = col % 2
    partner = (row, col + 1 - 2 * core)
    odd = (row + col // 2) % 2

    def at(start, size):
        return pl.ds(pl.multiple_of(start, 8), size)

    def lanes(start, size):
        return pl.ds(pl.multiple_of(start, min(128, size)), size)

    def remote(src, dst, send, recv, where):
        return pltpu.make_async_remote_copy(
            src_ref=src, dst_ref=dst, send_sem=send, recv_sem=recv, device_id=(spin,) + tuple(where), device_id_type=pl.DeviceIdType.MESH
        )

    others = [(dr, dc) for dr in range(4) for dc in range(4) if dr or dc]
    barrier = pltpu.get_barrier_semaphore()
    for dr, dc in others:
        pl.semaphore_signal(
            barrier, inc=1, device_id=(spin, (row + dr) % 4, (col + dc) % 4), device_id_type=pl.DeviceIdType.MESH
        )
    pl.semaphore_wait(barrier, len(others))

    def quadrant(src, which):
        low = jnp.where(src[0] > src[1], half, 0)
        return ((0, half), (low, low), (half, half))[which]

    def region(src, which):
        qr, qc = quadrant(src, which)
        return x_ref.at[1, at(src[0] * block + qr, half), lanes(src[1] * block + qc, half)]

    def own_region(which):
        qr, qc = quadrant((row, col), which)
        return h_ref.at[at(qr, half), lanes(qc, half)]

    def each(src, run, *conditions):
        for which in range(3):
            terms = list(conditions) + ([src[0] == src[1]] if which == 2 else [])
            if terms:
                pl.when(functools.reduce(jnp.logical_and, terms))(functools.partial(run, which))
            else:
                run(which)

    x_ref[1, at(row * block, block), lanes(col * block, block)] = h_ref[...]
    stage[...] = jnp.zeros_like(stage)
    far = (col + 2) % 4
    end = 3 * core

    def span(src, which, send, recv, n, where, own=False):
        spot = region(src, which)
        return remote(own_region(which) if own else spot, spot, send.at[3 * n + which], recv.at[3 * n + which], where)

    def z_out(turn, way, which):
        sign = 1 - 2 * way
        return span((row + sign * turn, col), which, z_send, z_recv, 2 * turn + way, (row - sign, col), turn == 0)

    def z_in(turn, way, which):
        sign = 1 - 2 * way
        return span((row + sign * turn, col), which, z_send, z_recv, 2 * (turn - 1) + way, (row + sign, col))

    def y_out(r, which, own=False):
        return span((r, col), which, y_send, y_recv, r, (row, far), own)

    def y_in(r, which):
        return span((r, far), which, y_send, y_recv, r, (row, far))

    def e_out(which):
        return span((end, far), which, e_send, e_recv, 0, (row + 1 - 2 * core, col))

    def e_in(which):
        return span((end, far), which, e_send, e_recv, 0, (row - 1 + 2 * core, col))

    def f_out(c, r, which, own=False):
        return span((r, c), which, f_send, f_recv, 4 * (c // 2) + r, partner, own)

    def f_in(c, r, which):
        return span((r, c + 1 - 2 * core), which, f_send, f_recv, 4 * (c // 2) + r, partner)

    def has(r):
        return jnp.logical_and(r >= 0, r <= 3)

    def crosses(r):
        return jnp.logical_or(r != end, row == end)

    def first(which):
        y_out(row, which, True).start()

        @pl.when(row > 0)
        def _():
            z_out(0, 0, which).start()

        @pl.when(row < 3)
        def _():
            z_out(0, 1, which).start()

        f_out(col, row, which, True).start()

    each((row, col), first)

    def take_line(turn):
        for way in range(2):
            sign = 1 - 2 * way
            r = row + sign * turn

            def arrived(which):
                z_in(turn, way, which).wait_recv()
                if turn < 3:
                    @pl.when(has(row - sign))
                    def _():
                        z_out(turn, way, which).start()

                @pl.when(crosses(r))
                def _():
                    y_out(r, which).start()

                f_out(col, r, which).start()

            each((r, col), arrived, has(r))

    def take_across(r):
        def arrived(which):
            y_in(r, which).wait_recv()
            f_out(far, r, which).start()

        each((r, far), arrived, has(r), crosses(r))

    def hand_on(which):
        @pl.when(has(row + 1 - 2 * core))
        def _():
            e_out(which).start()

    take_line(1)
    take_across(row)
    each((end, far), hand_on, row == end)
    take_line(2)
    take_across(row - 1)
    take_across(row + 1)
    take_line(3)

    def ended(which):
        e_in(which).wait_recv()
        hand_on(which)
        f_out(far, end, which).start()

    each((end, far), ended, row != end)
    for apart in (2, 3):
        take_across(row - apart)
        take_across(row + apart)
    for c in (col, far):
        for r in range(4):
            each((r, c + 1 - 2 * core), lambda which, c=c, r=r: f_in(c, r, which).wait_recv())

    def gather_drained():
        for c in (col, far):
            for r in range(4):
                each((r, c), lambda which, c=c, r=r: f_out(c, r, which).wait_send())
        for r in range(4):
            each((r, col), lambda which, r=r: y_out(r, which).wait_send(), crosses(r))
        for turn in range(3):
            for way in range(2):
                sign = 1 - 2 * way
                r = row + sign * turn
                each((r, col), lambda which, turn=turn, way=way: z_out(turn, way, which).wait_send(), has(r), has(row - sign))
        each((end, far), lambda which: e_out(which).wait_send(), has(row + 1 - 2 * core))

    gather_drained()

    quad_eye = lax.broadcasted_iota(jnp.int32, (half, half), 0) == lax.broadcasted_iota(jnp.int32, (half, half), 1)
    trace = jnp.zeros((half, half), F32)
    for k in range(8):
        trace = trace + x_ref[1, k * half:(k + 1) * half, k * half:(k + 1) * half]
    trace = jnp.where(quad_eye, trace, 0.0)
    chem = jnp.sum(jnp.sum(trace, axis=0, keepdims=True), axis=1, keepdims=True) / order
    occupied = jnp.full((1, 1), occ_ref[0], jnp.int32).astype(F32)
    scale = jnp.minimum(occupied / (bounds_ref[1] - chem), (order - occupied) / (chem - bounds_ref[0])) / order
    shift = occupied / order

    def convert(n, carry):
        i, j = n // 4, n % 4
        low = jnp.where(i > j, half, 0)

        def one(qr, qc):
            eye = jnp.logical_and(quad_eye, i * block + qr == j * block + qc)
            value = x_ref[1, at(i * block + qr, half), lanes(j * block + qc, half)]
            value = scale * (jnp.where(eye, chem, 0.0) - value) + jnp.where(eye, shift, 0.0)
            x_ref[0, at(i * block + qr, half), lanes(j * block + qc, half)] = value
            x_ref[0, at(j * block + qc, half), lanes(i * block + qr, half)] = value.T

        one(0, half)
        one(low, low)

        @pl.when(i == j)
        def _():
            one(half, half)

        return carry

    lax.fori_loop(0, 16, convert, 0)

    def sigma(flip, i):
        return i + flip * (3 - 2 * i)

    def between(flip, who):
        return sigma(flip, 0) * block + who * half, sigma(flip, 1) * block

    def single(flip, who):
        return who * block + half, (2 + who + flip * (1 - 2 * who)) * block

    def common(flip, who, k):
        return (who + flip * (k - who)) * block, (2 + k + flip * (1 - who - k)) * block

    def product(cur, r0, c0, height, width, flag):
        got = jnp.dot(
            x_ref[cur, at(r0, height), :], x_ref[cur, :, lanes(c0, width)], precision=lax.Precision.HIGHEST, preferred_element_type=F32
        )
        old = x_ref[cur, at(r0, height), lanes(c0, width)]
        return jnp.where(flag == 1, got, 2.0 * old - got)

    near = (neighbour(0, row, col), neighbour(2, row, col))
    sources = near + (partner,)

    def signal_credit():
        for n, where in enumerate(sources):
            pl.semaphore_signal(credit.at[n], inc=1, device_id=(spin,) + where, device_id_type=pl.DeviceIdType.MESH)

    def take_credit():
        for n in range(3):
            pl.semaphore_wait(credit.at[n], 1)

    def lane_sums(value):
        total = value[:, :128]
        for k in range(1, block // 128):
            total = total + value[:, k * 128:(k + 1) * 128]
        return jnp.sum(total, axis=0, keepdims=True)

    def squares(cur):
        own = x_ref[cur, at(row * block, block), lanes(col * block, block)]
        return lane_sums(own * own)

    quarter = half // 2

    def rect(slot, r0, c0, height, width):
        return x_ref.at[slot, at(r0, height), lanes(c0, width)]

    def piece(flip, who, k):
        d0 = sigma(flip, who) * block
        if k == 0:
            return d0, d0, block
        if k == 1:
            return d0 + half, d0 + half, half
        return (between if k == 2 else single)(flip, who) + (block,)

    def part_copy(flip, who, k, part, slot, send, recv, where):
        r0, c0, width = piece(flip, who, k)
        spot = rect(slot, r0 + part * quarter, c0, quarter, width)
        n = slot * 8 + k * 2 + part
        return remote(spot, spot, send.at[n], recv.at[n], where)

    def sender(who, k):
        return who + odd * (1 - 2 * who) if k == 3 else who

    def outward(k, part, slot):
        to_row, to_col = near[part]
        if k == 3:
            to_col = to_col + (1 - odd) * (1 - 2 * core)
        return part_copy(odd, core, k, part, slot, i_send, i_recv, (to_row, to_col))

    def inward(k, part, slot):
        return part_copy(1 - odd, sender(core, k), k, part, slot, i_send, i_recv, near[part])

    def passed(who, k, part, slot):
        return part_copy(1 - odd, sender(who, k), k, part, slot, w_send, w_recv, partner)

    def direct(who, k, slot):
        if k < 4:
            r0, c0, width = piece(odd, who, k)
        else:
            r0, c0 = common(odd, who, k - 4)
        if k == 0:
            spots = [rect(slot, r0, c0, half, block), rect(slot, c0 + half, r0, half, half)]
        elif k == 1:
            spots = [rect(slot, r0, c0, half, half)]
        else:
            spots = [rect(slot, r0, c0, half, block), rect(slot, c0, r0, block, half)]
        return [remote(spot, spot, d_send.at[slot * 12 + 2 * k + n], d_recv.at[slot * 12 + 2 * k + n], partner) for n, spot in enumerate(spots)]

    def send_piece(k, slot):
        if k < 4:
            for part in range(2):
                outward(k, part, slot).start()
        for copy in direct(core, k, slot):
            copy.start()

    def relay(k, slot):
        for part in range(2):
            inward(k, part, slot).wait_recv()
            passed(core, k, part, slot).start()

    def mirror(flip, who, k, slot):
        r0, c0, _ = piece(flip, who, k)
        if k == 0:
            x_ref[slot, at(c0 + half, half), lanes(r0, half)] = x_ref[slot, at(r0, half), lanes(c0 + half, half)].T
        else:
            x_ref[slot, at(c0, block), lanes(r0, half)] = x_ref[slot, at(r0, half), lanes(c0, block)].T

    def early(slot):
        relay(3, slot)
        for copy in direct(1 - core, 2, slot):
            copy.wait_recv()
        mirror(1 - odd, sender(core, 3), 3, slot)

    def settled(slot):
        relay(2, slot)
        for k in (0, 1, 3, 4, 5):
            for copy in direct(1 - core, k, slot):
                copy.wait_recv()
        for k in (0, 1, 3, 2):
            for part in range(2):
                passed(1 - core, k, part, slot).wait_recv()
        mirror(1 - odd, sender(1 - core, 3), 3, slot)
        for who in range(2):
            mirror(1 - odd, who, 0, slot)
            mirror(1 - odd, who, 2, slot)

    def drained(slot):
        for k in range(6):
            for copy in direct(core, k, slot):
                copy.wait_send()
        for k in range(4):
            for part in range(2):
                outward(k, part, slot).wait_send()
                passed(core, k, part, slot).wait_send()

    def work(u, carry):
        t, m = u // 5, u % 5
        cur, nxt = t % 2, 1 - t % 2
        flag = flag_ref[t]
        live = t < steps - 1

        def on(where, *conditions):
            for condition in conditions:
                where = jnp.logical_and(where, condition)
            return pl.when(where)

        @on(m == 0, t > 0)
        def _():
            early(cur)

        @on(m == 0, t == steps - 1)
        def _():
            settled(cur)
            stage[pl.ds(t, 1), :] = squares(cur)

        @on(m == 1, live)
        def _():
            r0, c0, _ = piece(odd, core, 1)
            x_ref[nxt, at(r0, half), lanes(c0, half)] = product(cur, r0, c0, half, half, flag)
            send_piece(1, nxt)

            @pl.when(t > 0)
            def _():
                settled(cur)

            stage[pl.ds(t, 1), :] = squares(cur)

        @on(m == 4)
        def _():
            relay(0, nxt)
            relay(1, nxt)

        d0 = piece(odd, core, 0)[:2]
        spots = (d0, single(odd, core), between(odd, core), common(odd, core, 0), common(odd, core, 1))
        r0, c0 = row * block + m * half, col * block
        for k, (r1, c1) in enumerate(spots):
            r0 = jnp.where(jnp.logical_and(live, m == k), r1, r0)
            c0 = jnp.where(jnp.logical_and(live, m == k), c1, c0)
        new = product(cur, r0, c0, half, block, flag)

        @on(m == 0, live)
        def _():
            take_credit()

        x_ref[nxt, at(r0, half), lanes(c0, block)] = new

        @pl.when(live)
        def _():
            x_ref[nxt, at(c0, block), lanes(r0, half)] = new.T

        for n, k in enumerate((0, 3, 2, 4, 5)):
            @on(m == n, live)
            def _():
                send_piece(k, nxt)

        @on(m == 4, t > 0)
        def _():
            drained(cur)

        @on(m == 4, t < steps - 2)
        def _():
            signal_credit()

        return carry

    signal_credit()
    lax.fori_loop(0, 5 * (steps - 1) + 2, work, 0)
    last = (steps - 1) % 2

    final = x_ref[1 - last, at(row * block, block), lanes(col * block, block)]
    dens_ref[...] = final
    stage[steps:steps + 1, :] = lane_sums(final * h_ref[...])
    drained(last)

    red[row * 4 + col] = stage[...]
    for n, (dr, dc) in enumerate(others):
        remote(stage, red.at[row * 4 + col], r_send.at[n], r_recv.at[n], ((row + dr) % 4, (col + dc) % 4)).start()
    for n, (dr, dc) in enumerate(others):
        spot = red.at[((row - dr) % 4) * 4 + (col - dc) % 4]
        remote(stage, spot, r_send.at[n], r_recv.at[n], partner).wait_recv()
    total = red[0]
    for n in range(1, 16):
        total = total + red[n]
    for n in range(steps):
        occs_ref[n] = jnp.sum(total[n:n + 1, :])
    energy_ref[0] = 2.0 * jnp.sum(total[steps:steps + 1, :])
    for n, (dr, dc) in enumerate(others):
        remote(stage, red.at[row * 4 + col], r_send.at[n], r_recv.at[n], ((row + dr) % 4, (col + dc) % 4)).wait_send()


def solution(mesh):
    def local_run(ham_block, bounds, occ_count, branches):
        block, steps = ham_block.shape[0], branches.shape[0]
        order = 4 * block
        dma = pltpu.SemaphoreType.DMA
        vmem = pl.BlockSpec(memory_space=pltpu.VMEM)
        smem = pl.BlockSpec(memory_space=pltpu.SMEM)
        return pl.pallas_call(
            functools.partial(kernel, steps),
            out_shape=(
                jax.ShapeDtypeStruct((block, block), F32),
                jax.ShapeDtypeStruct((steps,), F32),
                jax.ShapeDtypeStruct((1,), F32),
            ),
            in_specs=[vmem, smem, smem, smem],
            out_specs=(vmem, smem, smem),
            scratch_shapes=[
                pltpu.VMEM((2, order, order), F32),
                pltpu.VMEM((8, 128), F32),
                pltpu.VMEM((16, 8, 128), F32),
                dma((18,)), dma((18,)), dma((3,)), dma((3,)), dma((12,)), dma((12,)), dma((24,)), dma((24,)),
                dma((16,)), dma((16,)), dma((24,)), dma((24,)), dma((16,)), dma((16,)),
                dma((15,)), dma((15,)),
                pltpu.SemaphoreType.REGULAR((3,)),
            ],
            compiler_params=pltpu.CompilerParams(collective_id=0, has_side_effects=True, vmem_limit_bytes=60 * 1024 * 1024),
        )(ham_block, bounds, occ_count, branches)

    return jax.shard_map(
        local_run,
        mesh=mesh,
        in_specs=(P(("spin", "row"), "col"), P("spin"), P("spin"), P("spin")),
        out_specs=(P(("spin", "row"), "col"), P("spin"), P("spin")),
        check_vma=False,
    )
```

```python
import functools

import jax
import jax.numpy as jnp
from jax import lax
from jax.experimental import pallas as pl
from jax.experimental.pallas import tpu as pltpu
from jax.sharding import PartitionSpec as P

F32 = jnp.float32


def neighbour(dim, row, col):
    if dim == 0:
        return row + 1 - 2 * (row % 2), col
    return row, (col + 2) % 4


def kernel(steps, h_ref, bounds_ref, occ_ref, flag_ref, dens_ref, occs_ref, energy_ref, x_ref, stage, red, traces, t_send, t_recv, z_send, z_recv, e_send,
           e_recv, y_send, y_recv, f_send, f_recv, s_send, i_recv, h_recv, s_recv, r_send, r_recv, credit):
    block = h_ref.shape[0]
    half = block // 2
    order = 4 * block
    spin, row, col = lax.axis_index("spin"), lax.axis_index("row"), lax.axis_index("col")
    core = col % 2
    partner = (row, col + 1 - 2 * core)
    odd = (row + col // 2) % 2

    def at(start, size):
        return pl.ds(pl.multiple_of(start, 8), size)

    def lanes(start, size):
        return pl.ds(pl.multiple_of(start, min(128, size)), size)

    def remote(src, dst, send, recv, where):
        return pltpu.make_async_remote_copy(
            src_ref=src, dst_ref=dst, send_sem=send, recv_sem=recv, device_id=(spin,) + tuple(where), device_id_type=pl.DeviceIdType.MESH
        )

    others = [(dr, dc) for dr in range(4) for dc in range(4) if dr or dc]
    barrier = pltpu.get_barrier_semaphore()
    for dr, dc in others:
        pl.semaphore_signal(
            barrier, inc=1, device_id=(spin, (row + dr) % 4, (col + dc) % 4), device_id_type=pl.DeviceIdType.MESH
        )
    pl.semaphore_wait(barrier, len(others))

    def await_send(sem, units):
        spot = x_ref.at[0, pl.ds(0, units * (half * half) // order), :]
        remote(spot, spot, sem, h_recv.at[0], partner).wait_send()

    def await_recv(sem, units):
        spot = x_ref.at[0, pl.ds(0, units * (half * half) // order), :]
        remote(spot, spot, s_send.at[0], sem, partner).wait_recv()

    def quadrant(src, which):
        low = jnp.where(src[0] > src[1], half, 0)
        return ((0, half), (low, low), (half, half))[which]

    def region(src, which):
        qr, qc = quadrant(src, which)
        return x_ref.at[1, at(src[0] * block + qr, half), lanes(src[1] * block + qc, half)]

    def own_region(which):
        qr, qc = quadrant((row, col), which)
        return h_ref.at[at(qr, half), lanes(qc, half)]

    def each(src, run, *conditions):
        for which in range(3):
            terms = list(conditions) + ([src[0] == src[1]] if which == 2 else [])
            if terms:
                pl.when(functools.reduce(jnp.logical_and, terms))(functools.partial(run, which))
            else:
                run(which)

    x_ref[1, at(row * block, block), lanes(col * block, block)] = h_ref[...]
    far = (col + 2) % 4
    end = 3 * core

    def span(src, which, send, recv, n, where, own=False, merged=False):
        spot = region(src, which)
        recv_sem = recv.at[n] if merged else recv.at[3 * n + which]
        return remote(own_region(which) if own else spot, spot, send.at[0 if merged else n], recv_sem, where)

    def whole(src, wait):
        pl.when(src[0] == src[1])(lambda: wait(3))
        pl.when(src[0] != src[1])(lambda: wait(2))

    def z_out(turn, way, which):
        sign = 1 - 2 * way
        return span((row + sign * turn, col), which, z_send, z_recv, 2 * turn + way, (row - sign, col), turn == 0)

    def z_in(turn, way, which):
        sign = 1 - 2 * way
        return span((row + sign * turn, col), which, z_send, z_recv, 2 * (turn - 1) + way, (row + sign, col))

    def y_out(r, which, own=False):
        return span((r, col), which, y_send, y_recv, r, (row, far), own)

    def y_in(r, which):
        return span((r, far), which, y_send, y_recv, r, (row, far))

    def e_out(which):
        return span((end, far), which, e_send, e_recv, 0, (row + 1 - 2 * core, col))

    def e_in(which):
        return span((end, far), which, e_send, e_recv, 0, (row - 1 + 2 * core, col))

    def f_out(c, r, which, own=False):
        return span((r, c), which, f_send, f_recv, 4 * (c // 2) + r, partner, own, True)

    def has(r):
        return jnp.logical_and(r >= 0, r <= 3)

    def crosses(r):
        return jnp.logical_or(r != end, row == end)

    def first(which):
        y_out(row, which, True).start()

        @pl.when(row > 0)
        def _():
            z_out(0, 0, which).start()

        @pl.when(row < 3)
        def _():
            z_out(0, 1, which).start()

        f_out(col, row, which, True).start()

    quad_eye = lax.broadcasted_iota(jnp.int32, (half, half), 0) == lax.broadcasted_iota(jnp.int32, (half, half), 1)

    @pl.when(row == col)
    def _():
        diagonal = jnp.where(quad_eye, h_ref[:half, :half] + h_ref[half:, half:], 0.0)
        stage[...] = jnp.zeros_like(stage)
        for k in range(max(half // 128, 1)):
            stage[0:1, :min(half, 128)] += jnp.sum(diagonal[:, k * 128:(k + 1) * 128], axis=0, keepdims=True)
        traces[row] = stage[...]
        for n, (dr, dc) in enumerate(others):
            remote(stage, traces.at[row], t_send.at[0], t_recv.at[row], ((row + dr) % 4, (col + dc) % 4)).start()

    each((row, col), first)

    for k in range(4):
        @pl.when(jnp.logical_or(row != k, col != k))
        def _():
            remote(stage, traces.at[k], t_send.at[0], t_recv.at[k], partner).wait_recv()

    chem = jnp.sum(jnp.sum(traces[0] + traces[1] + traces[2] + traces[3], axis=0, keepdims=True), axis=1, keepdims=True) / order
    occupied = jnp.full((1, 1), occ_ref[0], jnp.int32).astype(F32)
    scale = jnp.minimum(occupied / (bounds_ref[1] - chem), (order - occupied) / (chem - bounds_ref[0])) / order
    shift = occupied / order

    def convert(r, c, *conditions):
        def body(which, carry):
            low = jnp.where(r > c, half, 0)
            qr = jnp.where(which == 0, 0, jnp.where(which == 1, low, half))
            qc = jnp.where(which == 0, half, qr)
            eye = jnp.logical_and(quad_eye, r * block + qr == c * block + qc)
            value = x_ref[1, at(r * block + qr, half), lanes(c * block + qc, half)]
            value = scale * (jnp.where(eye, chem, 0.0) - value) + jnp.where(eye, shift, 0.0)
            x_ref[0, at(r * block + qr, half), lanes(c * block + qc, half)] = value
            x_ref[0, at(c * block + qc, half), lanes(r * block + qr, half)] = value.T
            return carry

        def run():
            lax.fori_loop(0, 2 + jnp.where(r == c, 1, 0), body, 0)

        if conditions:
            pl.when(functools.reduce(jnp.logical_and, conditions))(run)
        else:
            run()

    def from_partner(c, r, *conditions):
        src = (r, c + 1 - 2 * core)

        def run():
            whole(src, lambda units: await_recv(f_recv.at[4 * (c // 2) + r], units))
            convert(*src)

        if conditions:
            pl.when(functools.reduce(jnp.logical_and, conditions))(run)
        else:
            run()

    def take_line(turn):
        for way in range(2):
            sign = 1 - 2 * way
            r = row + sign * turn

            def arrived(which):
                z_in(turn, way, which).wait_recv()
                if turn < 3:
                    @pl.when(has(row - sign))
                    def _():
                        z_out(turn, way, which).start()

                @pl.when(crosses(r))
                def _():
                    y_out(r, which).start()

                f_out(col, r, which).start()

            each((r, col), arrived, has(r))

    def take_across(r):
        def arrived(which):
            y_in(r, which).wait_recv()
            f_out(far, r, which).start()

        each((r, far), arrived, has(r), crosses(r))

    def hand_on(which):
        @pl.when(has(row + 1 - 2 * core))
        def _():
            e_out(which).start()

    convert(row, col)
    take_line(1)
    take_across(row)
    each((end, far), hand_on, row == end)
    from_partner(col, row)
    convert(row, far)
    for r in (row - 1, row + 1):
        convert(r, col, has(r))
    take_line(2)
    from_partner(far, row)
    for r in (row - 1, row + 1):
        take_across(r)
        from_partner(col, r, has(r))
        convert(r, far, has(r), crosses(r))
    for r in (row - 2, row + 2):
        convert(r, col, has(r))
    take_line(3)

    def ended(which):
        e_in(which).wait_recv()
        hand_on(which)
        f_out(far, end, which).start()

    each((end, far), ended, row != end)
    for r in (row - 1, row + 1):
        from_partner(far, r, has(r), r != 3 - end)
    for r in (row - 2, row + 2):
        from_partner(col, r, has(r))
    for r in (row - 2, row + 2):
        take_across(r)
        convert(r, far, has(r), crosses(r))
    convert(end, far, row != end)
    for r in (row - 3, row + 3):
        take_across(r)
        convert(r, col, has(r))
        from_partner(col, r, has(r))
    for r in (row - 2, row + 2):
        from_partner(far, r, has(r), r != 3 - end)
    from_partner(far, 3 - end, row != 3 - end)
    for r in (row - 3, row + 3):
        convert(r, far, has(r), crosses(r))
        from_partner(far, r, has(r), r != 3 - end)

    def gather_drained():
        await_send(f_send.at[0], 18)
        for r in range(4):
            pl.when(crosses(r))(lambda r=r: whole((r, col), lambda units: await_send(y_send.at[r], units)))
        for turn in range(3):
            for way in range(2):
                sign = 1 - 2 * way
                r = row + sign * turn
                pl.when(jnp.logical_and(has(r), has(row - sign)))(
                    lambda r=r, n=2 * turn + way: whole((r, col), lambda units: await_send(z_send.at[n], units)))
        pl.when(has(row + 1 - 2 * core))(lambda: whole((end, far), lambda units: await_send(e_send.at[0], units)))

        @pl.when(row == col)
        def _():
            remote(red.at[pl.ds(0, 15)], red.at[pl.ds(0, 15)], t_send.at[0], t_recv.at[row], partner).wait_send()

    gather_drained()
    stage[...] = jnp.zeros_like(stage)

    def sigma(flip, i):
        return i + flip * (3 - 2 * i)

    def between(flip, who):
        return sigma(flip, 0) * block + who * half, sigma(flip, 1) * block

    def single(flip, who):
        return who * block + half, (2 + who + flip * (1 - 2 * who)) * block

    def common(flip, who, k):
        return (who + flip * (k - who)) * block, (2 + k + flip * (1 - who - k)) * block

    def product(cur, r0, c0, height, width, flag):
        got = jnp.dot(
            x_ref[cur, at(r0, height), :], x_ref[cur, :, lanes(c0, width)], precision=lax.Precision.HIGHEST, preferred_element_type=F32
        )
        old = x_ref[cur, at(r0, height), lanes(c0, width)]
        return jnp.where(flag == 1, got, 2.0 * old - got)

    near = (neighbour(0, row, col), neighbour(2, row, col))
    sources = near + (partner,)

    def signal_credit():
        for n, where in enumerate(sources):
            pl.semaphore_signal(credit.at[n], inc=1, device_id=(spin,) + where, device_id_type=pl.DeviceIdType.MESH)

    def take_credit():
        for n in range(3):
            pl.semaphore_wait(credit.at[n], 1)

    def lane_sums(value):
        total = value[:, :128]
        for k in range(1, block // 128):
            total = total + value[:, k * 128:(k + 1) * 128]
        return jnp.sum(total, axis=0, keepdims=True)

    def squares(cur):
        own = x_ref[cur, at(row * block, block), lanes(col * block, block)]
        return lane_sums(own * own)

    quarter = half // 2

    def rect(slot, r0, c0, height, width):
        return x_ref.at[slot, at(r0, height), lanes(c0, width)]

    def piece(flip, who, k):
        d0 = sigma(flip, who) * block
        if k == 0:
            return d0, d0, block
        if k == 1:
            return d0 + half, d0 + half, half
        return (between if k == 2 else single)(flip, who) + (block,)

    def sender(who, k):
        return who + odd * (1 - 2 * who) if k == 3 else who

    def outward(k, slot):
        r0, c0, width = piece(odd, core, k)
        for part, (to_row, to_col) in enumerate(near):
            if k == 3:
                to_col = to_col + (1 - odd) * (1 - 2 * core)
            spot = rect(slot, r0 + part * quarter, c0, quarter, width)
            remote(spot, spot, s_send.at[slot], i_recv.at[slot * 4 + k], (to_row, to_col)).start()

    def to_partner(slot, r0, c0, height, width, sem):
        spot = rect(slot, r0, c0, height, width)
        remote(spot, spot, s_send.at[slot], sem, partner).start()

    def pair(k, r0, c0, slot, sem):
        to_partner(slot, r0, c0, half, half if k == 1 else block, sem)
        if k == 0:
            to_partner(slot, c0 + half, r0, half, half, sem)
        elif k != 1:
            to_partner(slot, c0, r0, block, half, sem)

    def send_piece(k, slot):
        if k < 4:
            outward(k, slot)
            r0, c0 = piece(odd, core, k)[:2]
        else:
            r0, c0 = common(odd, core, k - 4)
        pair(k, r0, c0, slot, (h_recv if k == 2 else s_recv).at[slot])

    def relay(k, slot):
        await_recv(i_recv.at[slot * 4 + k], 1 if k == 1 else 2)
        r0, c0, _ = piece(1 - odd, sender(core, k), k)
        if k == 0:
            x_ref[slot, at(c0 + half, half), lanes(r0, half)] = x_ref[slot, at(r0, half), lanes(c0 + half, half)].T
        elif k != 1:
            x_ref[slot, at(c0, block), lanes(r0, half)] = x_ref[slot, at(r0, half), lanes(c0, block)].T
        pair(k, r0, c0, slot, s_recv.at[slot])

    def early(slot):
        relay(3, slot)
        await_recv(h_recv.at[slot], 4)

    def settled(slot):
        await_recv(s_recv.at[slot], 28)

    def drained(slot):
        await_send(s_send.at[slot], 39)

    def work(u, carry):
        t, m = u // 5, u % 5
        cur, nxt = t % 2, 1 - t % 2
        flag = flag_ref[t]
        live = t < steps - 1

        def on(where, *conditions):
            for condition in conditions:
                where = jnp.logical_and(where, condition)
            return pl.when(where)

        @on(m == 0, t > 0)
        def _():
            early(cur)

        @on(m == 0, t == steps - 1)
        def _():
            relay(2, cur)
            settled(cur)
            stage[pl.ds(t, 1), :] = squares(cur)

        @on(m == 1, live)
        def _():
            @pl.when(t > 0)
            def _():
                relay(2, cur)

            r0, c0, _ = piece(odd, core, 1)
            x_ref[nxt, at(r0, half), lanes(c0, half)] = product(cur, r0, c0, half, half, flag)
            send_piece(1, nxt)

            @pl.when(t > 0)
            def _():
                settled(cur)

            stage[pl.ds(t, 1), :] = squares(cur)

        @on(m == 4)
        def _():
            relay(0, nxt)
            relay(1, nxt)

        d0 = piece(odd, core, 0)[:2]
        spots = (d0, single(odd, core), between(odd, core), common(odd, core, 0), common(odd, core, 1))
        r0, c0 = row * block + m * half, col * block
        for k, (r1, c1) in enumerate(spots):
            r0 = jnp.where(jnp.logical_and(live, m == k), r1, r0)
            c0 = jnp.where(jnp.logical_and(live, m == k), c1, c0)
        new = product(cur, r0, c0, half, block, flag)

        @on(m == 0, live)
        def _():
            take_credit()

        x_ref[nxt, at(r0, half), lanes(c0, block)] = new

        @pl.when(live)
        def _():
            x_ref[nxt, at(c0, block), lanes(r0, half)] = new.T

        for n, k in enumerate((0, 3, 2, 4, 5)):
            @on(m == n, live)
            def _():
                send_piece(k, nxt)

        @on(m == 4, t > 0)
        def _():
            drained(cur)

        @on(m == 4, t < steps - 2)
        def _():
            signal_credit()

        return carry

    signal_credit()
    lax.fori_loop(0, 5 * (steps - 1) + 2, work, 0)
    last = (steps - 1) % 2

    final = x_ref[1 - last, at(row * block, block), lanes(col * block, block)]
    dens_ref[...] = final
    stage[steps:steps + 1, :] = lane_sums(final * h_ref[...])
    drained(last)

    red[row * 4 + col] = stage[...]
    for n, (dr, dc) in enumerate(others):
        remote(stage, red.at[row * 4 + col], r_send.at[n], r_recv.at[n], ((row + dr) % 4, (col + dc) % 4)).start()
    for n, (dr, dc) in enumerate(others):
        spot = red.at[((row - dr) % 4) * 4 + (col - dc) % 4]
        remote(stage, spot, r_send.at[n], r_recv.at[n], partner).wait_recv()
    total = red[0]
    for n in range(1, 16):
        total = total + red[n]
    for n in range(steps):
        occs_ref[n] = jnp.sum(total[n:n + 1, :])
    energy_ref[0] = 2.0 * jnp.sum(total[steps:steps + 1, :])
    for n, (dr, dc) in enumerate(others):
        remote(stage, red.at[row * 4 + col], r_send.at[n], r_recv.at[n], ((row + dr) % 4, (col + dc) % 4)).wait_send()


def solution(mesh):
    def local_run(ham_block, bounds, occ_count, branches):
        block, steps = ham_block.shape[0], branches.shape[0]
        order = 4 * block
        dma = pltpu.SemaphoreType.DMA
        vmem = pl.BlockSpec(memory_space=pltpu.VMEM)
        smem = pl.BlockSpec(memory_space=pltpu.SMEM)
        return pl.pallas_call(
            functools.partial(kernel, steps),
            out_shape=(
                jax.ShapeDtypeStruct((block, block), F32),
                jax.ShapeDtypeStruct((steps,), F32),
                jax.ShapeDtypeStruct((1,), F32),
            ),
            in_specs=[vmem, smem, smem, smem],
            out_specs=(vmem, smem, smem),
            scratch_shapes=[
                pltpu.VMEM((2, order, order), F32),
                pltpu.VMEM((8, 128), F32),
                pltpu.VMEM((16, 8, 128), F32),
                pltpu.VMEM((4, 8, 128), F32),
                dma((1,)), dma((4,)), dma((6,)), dma((18,)), dma((1,)), dma((3,)), dma((4,)), dma((12,)), dma((1,)), dma((8,)),
                dma((2,)), dma((8,)), dma((2,)), dma((2,)),
                dma((15,)), dma((15,)),
                pltpu.SemaphoreType.REGULAR((3,)),
            ],
            compiler_params=pltpu.CompilerParams(collective_id=0, has_side_effects=True, vmem_limit_bytes=60 * 1024 * 1024),
        )(ham_block, bounds, occ_count, branches)

    return jax.shard_map(
        local_run,
        mesh=mesh,
        in_specs=(P(("spin", "row"), "col"), P("spin"), P("spin"), P("spin")),
        out_specs=(P(("spin", "row"), "col"), P("spin"), P("spin")),
        check_vma=False,
    )
```

```python
import functools

import jax
import jax.numpy as jnp
from jax import lax
from jax.experimental import pallas as pl
from jax.experimental.pallas import tpu as pltpu
from jax.sharding import PartitionSpec as P

F32 = jnp.float32


def neighbour(dim, row, col):
    if dim == 0:
        return row + 1 - 2 * (row % 2), col
    return row, (col + 2) % 4


def kernel(steps, h_hbm, bounds_ref, occ_ref, flag_ref, dens_hbm, occs_ref, energy_ref, h_ref, io_sem, x_ref, stage, red, traces, t_send, t_recv, z_send, z_recv, e_send,
           e_recv, y_send, y_recv, f_send, f_recv, s_send, i_recv, h_recv, s_recv, r_send, r_recv, credit):
    block = h_ref.shape[0]
    half = block // 2
    order = 4 * block
    spin, row, col = lax.axis_index("spin"), lax.axis_index("row"), lax.axis_index("col")
    core = col % 2
    partner = (row, col + 1 - 2 * core)
    odd = (row + col // 2) % 2

    def at(start, size):
        return pl.ds(pl.multiple_of(start, 8), size)

    def lanes(start, size):
        return pl.ds(pl.multiple_of(start, min(128, size)), size)

    def remote(src, dst, send, recv, where):
        return pltpu.make_async_remote_copy(
            src_ref=src, dst_ref=dst, send_sem=send, recv_sem=recv, device_id=(spin,) + tuple(where), device_id_type=pl.DeviceIdType.MESH
        )

    load = pltpu.make_async_copy(h_hbm, h_ref, io_sem.at[0])
    load.start()

    others = [(dr, dc) for dr in range(4) for dc in range(4) if dr or dc]
    barrier = pltpu.get_barrier_semaphore()
    for dr, dc in others:
        pl.semaphore_signal(
            barrier, inc=1, device_id=(spin, (row + dr) % 4, (col + dc) % 4), device_id_type=pl.DeviceIdType.MESH
        )
    load.wait()
    pl.semaphore_wait(barrier, len(others))

    def await_send(sem, units):
        spot = x_ref.at[0, pl.ds(0, units * (half * half) // order), :]
        remote(spot, spot, sem, h_recv.at[0], partner).wait_send()

    def await_recv(sem, units):
        spot = x_ref.at[0, pl.ds(0, units * (half * half) // order), :]
        remote(spot, spot, s_send.at[0], sem, partner).wait_recv()

    def quadrant(src, which):
        low = jnp.where(src[0] > src[1], half, 0)
        return ((0, half), (low, low), (half, half))[which]

    def region(src, which):
        qr, qc = quadrant(src, which)
        return x_ref.at[1, at(src[0] * block + qr, half), lanes(src[1] * block + qc, half)]

    def own_region(which):
        qr, qc = quadrant((row, col), which)
        return h_ref.at[at(qr, half), lanes(qc, half)]

    def each(src, run, *conditions):
        for which in range(3):
            terms = list(conditions) + ([src[0] == src[1]] if which == 2 else [])
            if terms:
                pl.when(functools.reduce(jnp.logical_and, terms))(functools.partial(run, which))
            else:
                run(which)

    x_ref[1, at(row * block, block), lanes(col * block, block)] = h_ref[...]
    far = (col + 2) % 4
    end = 3 * core

    def span(src, which, send, recv, n, where, own=False, merged=False):
        spot = region(src, which)
        recv_sem = recv.at[n] if merged else recv.at[3 * n + which]
        return remote(own_region(which) if own else spot, spot, send.at[0 if merged else n], recv_sem, where)

    def whole(src, wait):
        pl.when(src[0] == src[1])(lambda: wait(3))
        pl.when(src[0] != src[1])(lambda: wait(2))

    def z_out(turn, way, which):
        sign = 1 - 2 * way
        return span((row + sign * turn, col), which, z_send, z_recv, 2 * turn + way, (row - sign, col), turn == 0)

    def z_in(turn, way, which):
        sign = 1 - 2 * way
        return span((row + sign * turn, col), which, z_send, z_recv, 2 * (turn - 1) + way, (row + sign, col))

    def y_out(r, which, own=False):
        return span((r, col), which, y_send, y_recv, r, (row, far), own)

    def y_in(r, which):
        return span((r, far), which, y_send, y_recv, r, (row, far))

    def e_out(which):
        return span((end, far), which, e_send, e_recv, 0, (row + 1 - 2 * core, col))

    def e_in(which):
        return span((end, far), which, e_send, e_recv, 0, (row - 1 + 2 * core, col))

    def f_out(c, r, which, own=False):
        return span((r, c), which, f_send, f_recv, 4 * (c // 2) + r, partner, own, True)

    def has(r):
        return jnp.logical_and(r >= 0, r <= 3)

    def crosses(r):
        return jnp.logical_or(r != end, row == end)

    def first(which):
        y_out(row, which, True).start()

        @pl.when(row > 0)
        def _():
            z_out(0, 0, which).start()

        @pl.when(row < 3)
        def _():
            z_out(0, 1, which).start()

        f_out(col, row, which, True).start()

    quad_eye = lax.broadcasted_iota(jnp.int32, (half, half), 0) == lax.broadcasted_iota(jnp.int32, (half, half), 1)

    @pl.when(row == col)
    def _():
        diagonal = jnp.where(quad_eye, h_ref[:half, :half] + h_ref[half:, half:], 0.0)
        stage[...] = jnp.zeros_like(stage)
        for k in range(max(half // 128, 1)):
            stage[0:1, :min(half, 128)] += jnp.sum(diagonal[:, k * 128:(k + 1) * 128], axis=0, keepdims=True)
        traces[row] = stage[...]
        for n, (dr, dc) in enumerate(others):
            remote(stage, traces.at[row], t_send.at[0], t_recv.at[row], ((row + dr) % 4, (col + dc) % 4)).start()

    each((row, col), first)

    for k in range(4):
        @pl.when(jnp.logical_or(row != k, col != k))
        def _():
            remote(stage, traces.at[k], t_send.at[0], t_recv.at[k], partner).wait_recv()

    chem = jnp.sum(jnp.sum(traces[0] + traces[1] + traces[2] + traces[3], axis=0, keepdims=True), axis=1, keepdims=True) / order
    occupied = jnp.full((1, 1), occ_ref[0], jnp.int32).astype(F32)
    scale = jnp.minimum(occupied / (bounds_ref[1] - chem), (order - occupied) / (chem - bounds_ref[0])) / order
    shift = occupied / order

    def convert(r, c, *conditions):
        def body(which, carry):
            low = jnp.where(r > c, half, 0)
            qr = jnp.where(which == 0, 0, jnp.where(which == 1, low, half))
            qc = jnp.where(which == 0, half, qr)
            eye = jnp.logical_and(quad_eye, r * block + qr == c * block + qc)
            value = x_ref[1, at(r * block + qr, half), lanes(c * block + qc, half)]
            value = scale * (jnp.where(eye, chem, 0.0) - value) + jnp.where(eye, shift, 0.0)
            x_ref[0, at(r * block + qr, half), lanes(c * block + qc, half)] = value
            x_ref[0, at(c * block + qc, half), lanes(r * block + qr, half)] = value.T
            return carry

        def run():
            lax.fori_loop(0, 2 + jnp.where(r == c, 1, 0), body, 0)

        if conditions:
            pl.when(functools.reduce(jnp.logical_and, conditions))(run)
        else:
            run()

    def from_partner(c, r, *conditions):
        src = (r, c + 1 - 2 * core)

        def run():
            whole(src, lambda units: await_recv(f_recv.at[4 * (c // 2) + r], units))
            convert(*src)

        if conditions:
            pl.when(functools.reduce(jnp.logical_and, conditions))(run)
        else:
            run()

    def take_line(turn):
        for way in range(2):
            sign = 1 - 2 * way
            r = row + sign * turn

            def arrived(which):
                z_in(turn, way, which).wait_recv()
                if turn < 3:
                    @pl.when(has(row - sign))
                    def _():
                        z_out(turn, way, which).start()

                @pl.when(crosses(r))
                def _():
                    y_out(r, which).start()

                f_out(col, r, which).start()

            each((r, col), arrived, has(r))

    def take_across(r):
        def arrived(which):
            y_in(r, which).wait_recv()
            f_out(far, r, which).start()

        each((r, far), arrived, has(r), crosses(r))

    def hand_on(which):
        @pl.when(has(row + 1 - 2 * core))
        def _():
            e_out(which).start()

    convert(row, col)
    take_line(1)
    take_across(row)
    each((end, far), hand_on, row == end)
    from_partner(col, row)
    convert(row, far)
    for r in (row - 1, row + 1):
        convert(r, col, has(r))
    take_line(2)
    from_partner(far, row)
    for r in (row - 1, row + 1):
        take_across(r)
        from_partner(col, r, has(r))
        convert(r, far, has(r), crosses(r))
    for r in (row - 2, row + 2):
        convert(r, col, has(r))
    take_line(3)

    def ended(which):
        e_in(which).wait_recv()
        hand_on(which)
        f_out(far, end, which).start()

    each((end, far), ended, row != end)
    for r in (row - 1, row + 1):
        from_partner(far, r, has(r), r != 3 - end)
    for r in (row - 2, row + 2):
        from_partner(col, r, has(r))
    for r in (row - 2, row + 2):
        take_across(r)
        convert(r, far, has(r), crosses(r))
    convert(end, far, row != end)
    for r in (row - 3, row + 3):
        take_across(r)
        convert(r, col, has(r))
        from_partner(col, r, has(r))
    for r in (row - 2, row + 2):
        from_partner(far, r, has(r), r != 3 - end)
    from_partner(far, 3 - end, row != 3 - end)
    for r in (row - 3, row + 3):
        convert(r, far, has(r), crosses(r))
        from_partner(far, r, has(r), r != 3 - end)

    def gather_drained():
        await_send(f_send.at[0], 18)
        for r in range(4):
            pl.when(crosses(r))(lambda r=r: whole((r, col), lambda units: await_send(y_send.at[r], units)))
        for turn in range(3):
            for way in range(2):
                sign = 1 - 2 * way
                r = row + sign * turn
                pl.when(jnp.logical_and(has(r), has(row - sign)))(
                    lambda r=r, n=2 * turn + way: whole((r, col), lambda units: await_send(z_send.at[n], units)))
        pl.when(has(row + 1 - 2 * core))(lambda: whole((end, far), lambda units: await_send(e_send.at[0], units)))

        @pl.when(row == col)
        def _():
            remote(red.at[pl.ds(0, 15)], red.at[pl.ds(0, 15)], t_send.at[0], t_recv.at[row], partner).wait_send()

    gather_drained()
    stage[...] = jnp.zeros_like(stage)

    def sigma(flip, i):
        return i + flip * (3 - 2 * i)

    def between(flip, who):
        return sigma(flip, 0) * block + who * half, sigma(flip, 1) * block

    def single(flip, who):
        return who * block + half, (2 + who + flip * (1 - 2 * who)) * block

    def common(flip, who, k):
        return (who + flip * (k - who)) * block, (2 + k + flip * (1 - who - k)) * block

    def product(cur, r0, c0, height, width, flag):
        got = jnp.dot(
            x_ref[cur, at(r0, height), :], x_ref[cur, :, lanes(c0, width)], precision=lax.Precision.HIGHEST, preferred_element_type=F32
        )
        old = x_ref[cur, at(r0, height), lanes(c0, width)]
        return jnp.where(flag == 1, got, 2.0 * old - got)

    near = (neighbour(0, row, col), neighbour(2, row, col))
    sources = near + (partner,)

    def signal_credit():
        for n, where in enumerate(sources):
            pl.semaphore_signal(credit.at[n], inc=1, device_id=(spin,) + where, device_id_type=pl.DeviceIdType.MESH)

    def take_credit():
        for n in range(3):
            pl.semaphore_wait(credit.at[n], 1)

    def lane_sums(value):
        total = value[:, :128]
        for k in range(1, block // 128):
            total = total + value[:, k * 128:(k + 1) * 128]
        return jnp.sum(total, axis=0, keepdims=True)

    def squares(cur):
        own = x_ref[cur, at(row * block, block), lanes(col * block, block)]
        return lane_sums(own * own)

    quarter = half // 2

    def rect(slot, r0, c0, height, width):
        return x_ref.at[slot, at(r0, height), lanes(c0, width)]

    def piece(flip, who, k):
        d0 = sigma(flip, who) * block
        if k == 0:
            return d0, d0, block
        if k == 1:
            return d0 + half, d0 + half, half
        return (between if k == 2 else single)(flip, who) + (block,)

    def sender(who, k):
        return who + odd * (1 - 2 * who) if k == 3 else who

    def outward(k, slot):
        r0, c0, width = piece(odd, core, k)
        for part, (to_row, to_col) in enumerate(near):
            if k == 3:
                to_col = to_col + (1 - odd) * (1 - 2 * core)
            spot = rect(slot, r0 + part * quarter, c0, quarter, width)
            remote(spot, spot, s_send.at[slot], i_recv.at[slot * 4 + k], (to_row, to_col)).start()

    def to_partner(slot, r0, c0, height, width, sem):
        spot = rect(slot, r0, c0, height, width)
        remote(spot, spot, s_send.at[slot], sem, partner).start()

    def pair(k, r0, c0, slot, sem):
        to_partner(slot, r0, c0, half, half if k == 1 else block, sem)
        if k == 0:
            to_partner(slot, c0 + half, r0, half, half, sem)
        elif k != 1:
            to_partner(slot, c0, r0, block, half, sem)

    def send_piece(k, slot):
        if k < 4:
            outward(k, slot)
            r0, c0 = piece(odd, core, k)[:2]
        else:
            r0, c0 = common(odd, core, k - 4)
        pair(k, r0, c0, slot, (h_recv if k == 2 else s_recv).at[slot])

    def relay(k, slot):
        await_recv(i_recv.at[slot * 4 + k], 1 if k == 1 else 2)
        r0, c0, width = piece(1 - odd, sender(core, k), k)
        to_partner(slot, r0, c0, half, width, s_recv.at[slot])
        if k == 0:
            x_ref[slot, at(c0 + half, half), lanes(r0, half)] = x_ref[slot, at(r0, half), lanes(c0 + half, half)].T
            to_partner(slot, c0 + half, r0, half, half, s_recv.at[slot])
        elif k != 1:
            x_ref[slot, at(c0, block), lanes(r0, half)] = x_ref[slot, at(r0, half), lanes(c0, block)].T
            if k == 3:
                to_partner(slot, c0, r0, block, half, s_recv.at[slot])

    def early(slot):
        relay(3, slot)
        await_recv(h_recv.at[slot], 4)

    def settled(slot):
        await_recv(s_recv.at[slot], 26)
        r0, c0, _ = piece(1 - odd, 1 - core, 2)
        x_ref[slot, at(c0, block), lanes(r0, half)] = x_ref[slot, at(r0, half), lanes(c0, block)].T

    def drained(slot):
        await_send(s_send.at[slot], 37)

    def work(u, carry):
        t, m = u // 5, u % 5
        cur, nxt = t % 2, 1 - t % 2
        flag = flag_ref[t]
        live = t < steps - 1

        def on(where, *conditions):
            for condition in conditions:
                where = jnp.logical_and(where, condition)
            return pl.when(where)

        @on(m == 0, t > 0)
        def _():
            early(cur)

        @on(m == 0, t == steps - 1)
        def _():
            relay(2, cur)
            settled(cur)
            stage[pl.ds(t, 1), :] = squares(cur)

        @on(m == 1, live)
        def _():
            @pl.when(t > 0)
            def _():
                relay(2, cur)

            r0, c0, _ = piece(odd, core, 1)
            x_ref[nxt, at(r0, half), lanes(c0, half)] = product(cur, r0, c0, half, half, flag)
            send_piece(1, nxt)

            @pl.when(t > 0)
            def _():
                settled(cur)

            stage[pl.ds(t, 1), :] = squares(cur)

        @on(m == 4)
        def _():
            relay(0, nxt)
            relay(1, nxt)

        d0 = piece(odd, core, 0)[:2]
        spots = (d0, single(odd, core), between(odd, core), common(odd, core, 0), common(odd, core, 1))
        r0, c0 = row * block + m * half, col * block
        for k, (r1, c1) in enumerate(spots):
            r0 = jnp.where(jnp.logical_and(live, m == k), r1, r0)
            c0 = jnp.where(jnp.logical_and(live, m == k), c1, c0)
        new = product(cur, r0, c0, half, block, flag)

        @on(m == 0, live)
        def _():
            take_credit()

        x_ref[nxt, at(r0, half), lanes(c0, block)] = new

        @pl.when(live)
        def _():
            x_ref[nxt, at(c0, block), lanes(r0, half)] = new.T

        for n, k in enumerate((0, 3, 2, 4, 5)):
            @on(m == n, live)
            def _():
                send_piece(k, nxt)

        @on(m == 4, t > 0)
        def _():
            drained(cur)

        @on(m == 4, t < steps - 2)
        def _():
            signal_credit()

        return carry

    signal_credit()
    lax.fori_loop(0, 5 * (steps - 1) + 2, work, 0)
    last = (steps - 1) % 2

    final = x_ref[1 - last, at(row * block, block), lanes(col * block, block)]
    stage[steps:steps + 1, :] = lane_sums(final * h_ref[...])
    store = pltpu.make_async_copy(x_ref.at[1 - last, at(row * block, block), lanes(col * block, block)], dens_hbm, io_sem.at[1])
    store.start()
    drained(last)

    red[row * 4 + col] = stage[...]
    for n, (dr, dc) in enumerate(others):
        remote(stage, red.at[row * 4 + col], r_send.at[n], r_recv.at[n], ((row + dr) % 4, (col + dc) % 4)).start()
    for n, (dr, dc) in enumerate(others):
        spot = red.at[((row - dr) % 4) * 4 + (col - dc) % 4]
        remote(stage, spot, r_send.at[n], r_recv.at[n], partner).wait_recv()
    total = red[0]
    for n in range(1, 16):
        total = total + red[n]
    for n in range(steps):
        occs_ref[n] = jnp.sum(total[n:n + 1, :])
    energy_ref[0] = 2.0 * jnp.sum(total[steps:steps + 1, :])
    for n, (dr, dc) in enumerate(others):
        remote(stage, red.at[row * 4 + col], r_send.at[n], r_recv.at[n], ((row + dr) % 4, (col + dc) % 4)).wait_send()
    store.wait()


def solution(mesh):
    def local_run(ham_block, bounds, occ_count, branches):
        block, steps = ham_block.shape[0], branches.shape[0]
        order = 4 * block
        dma = pltpu.SemaphoreType.DMA
        hbm = pl.BlockSpec(memory_space=pl.ANY)
        smem = pl.BlockSpec(memory_space=pltpu.SMEM)
        return pl.pallas_call(
            functools.partial(kernel, steps),
            out_shape=(
                jax.ShapeDtypeStruct((block, block), F32),
                jax.ShapeDtypeStruct((steps,), F32),
                jax.ShapeDtypeStruct((1,), F32),
            ),
            in_specs=[hbm, smem, smem, smem],
            out_specs=(hbm, smem, smem),
            scratch_shapes=[
                pltpu.VMEM((block, block), F32),
                dma((2,)),
                pltpu.VMEM((2, order, order), F32),
                pltpu.VMEM((8, 128), F32),
                pltpu.VMEM((16, 8, 128), F32),
                pltpu.VMEM((4, 8, 128), F32),
                dma((1,)), dma((4,)), dma((6,)), dma((18,)), dma((1,)), dma((3,)), dma((4,)), dma((12,)), dma((1,)), dma((8,)),
                dma((2,)), dma((8,)), dma((2,)), dma((2,)),
                dma((15,)), dma((15,)),
                pltpu.SemaphoreType.REGULAR((3,)),
            ],
            compiler_params=pltpu.CompilerParams(collective_id=0, has_side_effects=True, vmem_limit_bytes=60 * 1024 * 1024),
        )(ham_block, bounds, occ_count, branches)

    return jax.shard_map(
        local_run,
        mesh=mesh,
        in_specs=(P(("spin", "row"), "col"), P("spin"), P("spin"), P("spin")),
        out_specs=(P(("spin", "row"), "col"), P("spin"), P("spin")),
        check_vma=False,
    )
```
